128 devices in a mesh: walk: 8 (over y, x_lo), orb: 16 (over x_hi, z, core).
Axes of the slice: x: 4 (x_hi: 2, x_lo: 2; x = x_hi * 2 + x_lo), y: 4, z: 4, core: 2. Of those that a mesh axis runs over, the one named last changes fastest.
Arguments:
- coefficients: bfloat16 [4096, 4096], P(None, 'orb'), may hold values from -6 to 6
- inverse: bfloat16 [8, 1024, 1024], P('walk', 'orb'), may hold values from -0.005859375 to 0.005859375
- cell_index: int32 [8, 3, 1024], P('walk'), may hold values from 0 to 15
- fraction: float32 [8, 3, 1024], P('walk'), may hold values from 0 to 1
- energies: float32 [8], P('walk'), may hold values from -8 to 8
- weights: float32 [8], P('walk'), may hold values from 0.5 to 2
- occupied: int32 [1024], replicated, may hold values from 0 to 4095, as said below
Outputs:
- gradient: float32 [1024, 4096], P('walk', 'orb')
The draws below stay inside these ranges and needn't reach their ends.
Inputs may be any that keep to these rules, and one draw needn't show every extreme that they name: `occupied`: 1024 distinct orbital indices; every block of 256 consecutive orbital indices holds at most 96 of them, and some block holds exactly 96.
All inputs are finite; a program needn't handle non-finite values.
Results may differ from the reference program's by a relative error of at most 0.019.
Values may be sent and summed in bfloat16 or wider, within the bound.
A program may use at most 64 MiB of HBM per device.

```python
import math
import jax
import jax.numpy as jnp
from jax import lax

N = 1024
M = 4096
GRID = 16
SAMPLES = 8
CELLS = 4096
N_ORB = 16


def draw_occupied(key, part):
    shards = N_ORB
    local = M // N_ORB
    bound = 3 * N // (2 * N_ORB)
    others = shards - 1
    remainder = N - bound
    base = remainder // others
    extra = remainder - base * others
    key_moves = jax.random.fold_in(key, 11)
    key_spot = jax.random.fold_in(key, 12)
    key_score = jax.random.fold_in(key, 13)
    key_order = jax.random.fold_in(key, 14)
    counts = base + (jnp.arange(others, dtype=jnp.int32) < extra).astype(jnp.int32)
    margin = max(0, min(base - 1, bound - base - 2))
    pairs = others // 2
    moves = jax.random.randint(key_moves, (pairs,), 0, margin + 1).astype(jnp.int32)
    change = jnp.zeros((others,), jnp.int32)
    change = change.at[0:2 * pairs:2].add(moves)
    change = change.at[1:2 * pairs:2].add(-moves)
    counts = counts + change
    full = jnp.concatenate([jnp.full((1,), bound, jnp.int32), counts])
    spot = jax.random.randint(key_spot, (), 0, shards)
    full = jnp.roll(full, spot)
    scores = jax.random.randint(key_score, (shards, local), 0, 1 << 20).astype(jnp.int32) * local + jnp.arange(local, dtype=jnp.int32)[None, :]
    scores = scores.at[0, 0].set(-1)
    scores = scores.at[shards - 1, local - 1].set(-1)
    ranking = jnp.argsort(jnp.argsort(scores, axis=1), axis=1).astype(jnp.int32)
    chosen = (ranking < full[:, None]).reshape(-1)
    orbital_ids = jnp.arange(shards * local, dtype=jnp.int32)
    keyed = jnp.where(chosen, orbital_ids, orbital_ids + shards * local)
    picked = jnp.sort(keyed)[:N]
    return jax.random.permutation(key_order, picked).astype(jnp.int32)


def with_ends(array, key, low, top_value):
    spot = [jax.random.randint(jax.random.fold_in(key, axis), (), 0, length) for axis, length in enumerate(array.shape)]
    main_axis = array.shape.index(max(array.shape))
    neighbour = spot[:main_axis] + [(spot[main_axis] + 1) % array.shape[main_axis]] + spot[main_axis + 1:]
    return array.at[tuple(spot)].set(low).at[tuple(neighbour)].set(top_value)


def block_levels(stream_key, dims, pieces, low, top_value):
    gain = 1.0
    for axis_at, shards_of in pieces:
        steps = jax.random.uniform(jax.random.fold_in(jax.random.fold_in(stream_key, 6), axis_at), (shards_of,), jnp.float32, low / len(pieces), top_value / len(pieces))
        gain = gain * jnp.repeat(jnp.exp(steps), dims[axis_at] // shards_of).reshape((-1,) + (1,) * (len(dims) - 1 - axis_at))
    return gain


def gaussian(stream_key, shape, deviation, most, cuts=(), held_as=jnp.bfloat16):
    result = jax.random.normal(stream_key, shape, jnp.float32) * deviation
    if len(cuts) > 0:
        result = block_levels(stream_key, shape, cuts, -0.22, 0.18) * result
    return jnp.clip(result, min=-most, max=most).astype(held_as)


def setup_inputs(seed: int = 0) -> dict:
    seeds = jax.random.split(jax.random.key(seed), 8)
    coefficients = gaussian(seeds[0], (CELLS, M), 1.0, 6.0, ((1, 16),))
    inverse = gaussian(seeds[1], (SAMPLES, N, N), (N * N) ** -0.5, 0.005859375, ((0, 8), (1, 16)))
    cell_index = with_ends(jax.random.randint(seeds[2], (SAMPLES, 3, N), 0, GRID), jax.random.fold_in(seeds[2], 1), 0, GRID - 1).astype(jnp.int32)
    fraction = jnp.clip(1.0 * jax.random.uniform(seeds[3], (SAMPLES, 3, N), jnp.float32) ** block_levels(seeds[3], (SAMPLES, 3, N), ((0, 8),), -0.2, 0.2), 0.0, 1.0)
    energies = gaussian(seeds[4], (SAMPLES,), 2.0, 8.0, ((0, 8),), jnp.float32)
    weights = jnp.clip(jnp.exp(math.log(2.0) - 1.3862944 * jax.random.uniform(seeds[5], (SAMPLES,), jnp.float32) ** block_levels(seeds[5], (SAMPLES,), ((0, 8),), -0.2, 0.2)), 0.5, 2.0)
    occupied = draw_occupied(jax.random.fold_in(seeds[7], 71), 0)
    return dict(coefficients=coefficients, inverse=inverse, cell_index=cell_index, fraction=fraction, energies=energies, weights=weights, occupied=occupied)


def spline_basis(frac):
    remain = 1.0 - frac
    square = frac * frac
    cubed = square * frac
    values = jnp.stack([remain * remain * remain, 3.0 * cubed - 6.0 * square + 4.0, -3.0 * cubed + 3.0 * square + 3.0 * frac + 1.0, cubed]) / 6.0
    curves = jnp.stack([remain, 3.0 * frac - 2.0, 1.0 - 3.0 * frac, frac])
    return values, curves


def evaluate(coefficients, cell_one, frac_one, edge):
    shifts = jnp.arange(4, dtype=jnp.int32)[:, None] - 1
    index_x = (cell_one[0][None, :] + shifts) % edge
    index_y = (cell_one[1][None, :] + shifts) % edge
    index_z = (cell_one[2][None, :] + shifts) % edge
    value_x, curve_x = spline_basis(frac_one[0])
    value_y, curve_y = spline_basis(frac_one[1])
    value_z, curve_z = spline_basis(frac_one[2])
    plane = (index_y[:, None, :] * edge + index_z[None, :, :]).reshape(16, -1)
    value_yz = (value_y[:, None, :] * value_z[None, :, :]).reshape(16, -1)
    curve_yz = (curve_y[:, None, :] * value_z[None, :, :] + value_y[:, None, :] * curve_z[None, :, :]).reshape(16, -1)
    electrons = cell_one.shape[1]
    orbital_sum = jnp.zeros((electrons, coefficients.shape[1]), jnp.float32)
    laplace_sum = jnp.zeros((electrons, coefficients.shape[1]), jnp.float32)
    for tap_x in range(4):
        tap_rows = index_x[tap_x][None, :] * (edge * edge) + plane
        tap_coef = jnp.take(coefficients, tap_rows, axis=0).astype(jnp.float32)
        weight_val = value_x[tap_x][None, :] * value_yz
        weight_lap = curve_x[tap_x][None, :] * value_yz + value_x[tap_x][None, :] * curve_yz
        orbital_sum = orbital_sum + jnp.einsum("kn,knw->nw", weight_val, tap_coef, precision=lax.Precision.HIGHEST)
        laplace_sum = laplace_sum + jnp.einsum("kn,knw->nw", weight_lap, tap_coef, precision=lax.Precision.HIGHEST)
    return orbital_sum.astype(jnp.bfloat16), laplace_sum.astype(jnp.bfloat16)


def wide_dot(left, right):
    return jnp.dot(left.astype(jnp.float32), right.astype(jnp.float32), precision=lax.Precision.HIGHEST)


def reference(coefficients, inverse, cell_index, fraction, energies, weights, occupied):
    def one_sample(running, items):
        inverse_one, cells_one, frac_one, energy, weight = items
        orbital_vals, laplace_vals = evaluate(coefficients, cells_one, frac_one, GRID)
        ratio = wide_dot(inverse_one, orbital_vals).astype(jnp.bfloat16)
        kinetic = wide_dot(inverse_one, laplace_vals)
        occupied_block = jnp.take(kinetic, occupied, axis=1).astype(jnp.bfloat16)
        coupled = wide_dot(occupied_block, ratio)
        sample_term = weight * (energy * ratio.astype(jnp.float32) - 0.5 * (kinetic - coupled))
        return running + sample_term, None

    initial = jnp.zeros((N, M), jnp.float32)
    gradient, unused = lax.scan(one_sample, initial, (inverse, cell_index, fraction, energies, weights))
    return gradient
```

```python
import jax
import jax.numpy as jnp
from jax import lax
from jax.experimental import pallas as pl
from jax.experimental.pallas import tpu as pltpu
from jax.sharding import PartitionSpec as P

MESH = pl.DeviceIdType.MESH
GRID = 16
N = 1024
WIDE = 256
CAP = 96
ROWS = 64
PLANE = GRID * GRID
ETILE = 512
GROUP = 4
COPIES = 19

NT = (((1,), (1,)), ((), ()))


def dot_nt(left, right):
    return lax.dot_general(left, right, NT, preferred_element_type=jnp.float32)


def dot_nn(left, right):
    return jnp.dot(left, right, preferred_element_type=jnp.float32)


def axis_table(cell, frac):
    remain = 1.0 - frac
    square = frac * frac
    cubed = square * frac
    sixth = 1.0 / 6.0
    values = (
        remain * remain * remain * sixth,
        (3.0 * cubed - 6.0 * square + 4.0) * sixth,
        (-3.0 * cubed + 3.0 * square + 3.0 * frac + 1.0) * sixth,
        cubed * sixth,
    )
    curves = (remain, 3.0 * frac - 2.0, 1.0 - 3.0 * frac, frac)
    tap = (lax.broadcasted_iota(jnp.int32, (GRID, N), 0) - cell + (GRID + 1)) & (GRID - 1)
    value = jnp.zeros((GRID, N), jnp.float32)
    curve = jnp.zeros((GRID, N), jnp.float32)
    for a in range(4):
        hit = tap == a
        value = jnp.where(hit, values[a], value)
        curve = jnp.where(hit, curves[a], curve)
    return value, curve


def slots_of(occ):
    block = occ >> 8
    member = (lax.broadcasted_iota(jnp.int32, (16, N), 0) == block).astype(jnp.float32)
    tiles = [member[:, t * 128 : (t + 1) * 128] for t in range(N // 128)]
    stacked = jnp.concatenate(tiles, axis=0).astype(jnp.bfloat16)
    row = lax.broadcasted_iota(jnp.int32, (128, 256), 0)
    col = lax.broadcasted_iota(jnp.int32, (128, 256), 1)
    upper = jnp.where((row < col) | (col >= 128), 1.0, 0.0).astype(jnp.bfloat16)
    counted = dot_nn(stacked, upper)
    before = jnp.zeros((16, 128), jnp.float32)
    ranks = []
    for t in range(N // 128):
        piece = counted[t * 16 : (t + 1) * 16, :]
        ranks.append(jnp.sum(tiles[t] * (piece[:, :128] + before), axis=0, keepdims=True))
        before = before + piece[:, 128:]
    return block * CAP + jnp.concatenate(ranks, axis=1).astype(jnp.int32)


def one_hot_rows(first, count, which):
    rows = lax.broadcasted_iota(jnp.int32, (count, N), 0) + first
    return jnp.where(rows == which, 1.0, 0.0).astype(jnp.bfloat16)


class Gather:
    def __init__(self, own, buf, rows, send, recv, place):
        self.own, self.buf, self.rows, self.send, self.recv = own, buf, rows, send, recv
        self.xh, self.z, self.c = place
        self.started = []

    def block(self, dx, dz, dc, part=None):
        xh = 1 - self.xh if dx else self.xh
        c = 1 - self.c if dc else self.c
        z = (self.z + dz) % 4
        half = self.rows // 2
        size = self.rows if part is None else half
        first = (xh * 8 + z * 2 + c) * self.rows + (0 if part is None else part * half)
        return self.buf.at[pl.ds(pl.multiple_of(first, 16), size), :]

    def device(self, name):
        xh, z, c = self.xh, self.z, self.c
        if name == "zp":
            z = (z + 1) % 4
        if name == "zm":
            z = (z + 3) % 4
        if name == "x":
            xh = 1 - xh
        if name == "s":
            c = 1 - c
        return {"orb": xh * 8 + z * 2 + c}

    def push(self, src, dst, to, at):
        copy = pltpu.make_async_remote_copy(
            src_ref=src,
            dst_ref=dst,
            send_sem=self.send.at[at],
            recv_sem=self.recv.at[at],
            device_id=self.device(to),
            device_id_type=MESH,
        )
        copy.start()
        self.started.append(copy)

    def arrived(self, spot, frm, at):
        here = self.block(*spot)
        pltpu.make_async_remote_copy(
            src_ref=here,
            dst_ref=here,
            send_sem=self.send.at[at],
            recv_sem=self.recv.at[at],
            device_id=self.device(frm),
            device_id_type=MESH,
        ).wait_recv()
        return here

    def start_own(self):
        mine = self.block(0, 0, 0)
        for at, to in enumerate(("zp", "zm", "x", "s")):
            self.push(self.own, mine, to, at)

    def near_z(self):
        got = self.arrived((0, 3, 0), "zm", 0)
        half = self.block(0, 3, 0, 0)
        self.push(half, half, "zp", 4)
        self.push(got, got, "s", 10)
        got = self.arrived((0, 1, 0), "zp", 1)
        half = self.block(0, 1, 0, 1)
        self.push(half, half, "zm", 5)
        self.push(got, got, "s", 11)

    def near_x(self):
        got = self.arrived((1, 0, 0), "x", 2)
        self.push(got, got, "zp", 6)
        self.push(got, got, "zm", 7)
        self.push(got, got, "s", 12)

    def far_z(self):
        got = self.arrived((0, 2, 0, 0), "zm", 4)
        self.push(got, got, "x", 8)
        self.push(got, got, "s", 13)
        got = self.arrived((0, 2, 0, 1), "zp", 5)
        self.push(got, got, "x", 9)
        self.push(got, got, "s", 14)

    def cross(self):
        got = self.arrived((1, 3, 0), "zm", 6)
        self.push(got, got, "s", 15)
        got = self.arrived((1, 1, 0), "zp", 7)
        self.push(got, got, "s", 16)

    def far_cross(self):
        got = self.arrived((1, 2, 0, 0), "x", 8)
        self.push(got, got, "s", 17)
        got = self.arrived((1, 2, 0, 1), "x", 9)
        self.push(got, got, "s", 18)

    def from_partner(self):
        spots = {
            3: (0, 0, 1),
            10: (0, 3, 1),
            11: (0, 1, 1),
            12: (1, 0, 1),
            13: (0, 2, 1, 0),
            14: (0, 2, 1, 1),
            15: (1, 3, 1),
            16: (1, 1, 1),
            17: (1, 2, 1, 0),
            18: (1, 2, 1, 1),
        }
        for at, spot in spots.items():
            self.arrived(spot, "s", at)

    def drain(self):
        for copy in self.started:
            copy.wait_send()


def kernel(
    coef_hbm,
    inv_ref,
    cell_ref,
    frac_ref,
    energy_ref,
    weight_ref,
    occ_ref,
    out_ref,
    coef,
    coef_t,
    plane_val,
    plane_lap,
    x_val,
    x_lap,
    stage,
    lap_t,
    val_t,
    inv_all,
    occ_all,
    ratio_t,
    slot_t,
    y_t,
    outgoing,
    incoming,
    load_sem,
    inv_send,
    inv_recv,
    occ_send,
    occ_recv,
    red_send,
    red_recv,
):
    walk, orb = lax.axis_index("walk"), lax.axis_index("orb")
    yy, xl = walk // 2, walk % 2
    place = (orb // 8, (orb // 2) % 4, orb % 2)
    load = pltpu.make_async_copy(coef_hbm, coef, load_sem)
    load.start()
    inv_gather = Gather(inv_ref, inv_all, ROWS, inv_send, inv_recv, place)
    mine = occ_all.at[pl.ds(pl.multiple_of(orb * CAP, 16), CAP), :]
    occ_gather = Gather(mine, occ_all, CAP, occ_send, occ_recv, place)
    steps = ((2, 1), (2, 0), (1, 1), (1, 0), (3, 1), (3, 0), (0, 1))

    def walk_of(dy, dx):
        return ((yy + dy) % 4) * 2 + (1 - xl if dx else xl)

    barrier = pltpu.get_barrier_semaphore()
    for name in ("zp", "zm", "x", "s"):
        pl.semaphore_signal(
            barrier, inc=1, device_id=inv_gather.device(name), device_id_type=MESH
        )
    for dy, dx in steps:
        pl.semaphore_signal(
            barrier, inc=1, device_id={"walk": walk_of(dy, dx)}, device_id_type=MESH
        )
    pl.semaphore_wait(barrier, 4 + len(steps))
    inv_gather.start_own()

    bx, cx = axis_table(cell_ref[0:1, :], frac_ref[0:1, :])
    by, cy = axis_table(cell_ref[1:2, :], frac_ref[1:2, :])
    bz, cz = axis_table(cell_ref[2:3, :], frac_ref[2:3, :])
    x_val[...] = bx
    x_lap[...] = cx
    for y in range(GRID):
        rows = slice(y * GRID, (y + 1) * GRID)
        plane_val[rows, :] = by[y : y + 1, :] * bz
        plane_lap[rows, :] = cy[y : y + 1, :] * bz + by[y : y + 1, :] * cz
    inv_all[pl.ds(pl.multiple_of(orb * ROWS, 16), ROWS), :] = inv_ref[...]
    occ = occ_ref[...]
    slot = slots_of(occ)
    pick = dot_nt(one_hot_rows(orb * CAP, CAP, slot), one_hot_rows(orb * WIDE, WIDE, occ))
    pick = pick.astype(jnp.bfloat16)
    load.wait()
    for x in range(GRID):
        points = slice(x * PLANE, (x + 1) * PLANE)
        coef_t[:, points] = coef[points, :].T

    def spline(cols, lap):
        total = None
        for g in range(GRID // GROUP):
            for k in range(GROUP):
                x = g * GROUP + k
                if lap:
                    piece = (
                        x_lap[x : x + 1, cols] * plane_val[:, cols]
                        + x_val[x : x + 1, cols] * plane_lap[:, cols]
                    )
                else:
                    piece = x_val[x : x + 1, cols] * plane_val[:, cols]
                stage[g % 2, k * PLANE : (k + 1) * PLANE, :] = piece.astype(jnp.bfloat16)
            part = dot_nn(
                coef_t[:, g * GROUP * PLANE : (g + 1) * GROUP * PLANE], stage[g % 2]
            )
            total = part if total is None else total + part
        return total.astype(jnp.bfloat16)

    tiles = [slice(t * ETILE, (t + 1) * ETILE) for t in range(N // ETILE)]
    for cols in tiles:
        lap_t[:, cols] = spline(cols, True)
    mine[...] = dot_nn(pick, lap_t[...]).astype(jnp.bfloat16)
    inv_gather.near_z()
    occ_gather.start_own()
    inv_gather.near_x()
    val_t[:, tiles[0]] = spline(tiles[0], False)
    inv_gather.far_z()
    val_t[:, tiles[1]] = spline(tiles[1], False)
    inv_gather.cross()
    inv_gather.far_cross()
    occ_gather.near_z()
    occ_gather.near_x()
    inv_gather.from_partner()
    ratio_t[...] = dot_nt(val_t[...], inv_all[...]).astype(jnp.bfloat16)
    occ_gather.far_z()
    for t in range(3):
        hot = one_hot_rows(t * 512, 512, slot)
        slot_t[:, t * 512 : (t + 1) * 512] = dot_nt(ratio_t[...], hot).astype(jnp.bfloat16)
    occ_gather.cross()
    occ_gather.far_cross()
    occ_gather.from_partner()

    weight = weight_ref[0]
    scaled = weight * energy_ref[0]
    half = 0.5 * weight
    for cols in tiles:
        coupled = dot_nn(slot_t[...], occ_all[:, cols])
        y_t[:, cols] = (
            scaled * val_t[:, cols].astype(jnp.float32)
            + half * (coupled - lap_t[:, cols].astype(jnp.float32))
        ).astype(jnp.bfloat16)

    sends = []
    own = None
    for dy in (2, 1, 3, 0):
        first = pl.multiple_of(((yy + dy) % 4) * 256, 256)
        terms = dot_nt(inv_all[pl.ds(first, 256), :], y_t[...])
        outgoing[pl.ds(first, 256), :] = terms.astype(jnp.bfloat16)
        for dx in (1, 0):
            if (dy, dx) == (0, 0):
                own = jnp.where(xl == 0, terms[:128, :], terms[128:, :])
                continue
            at = steps.index((dy, dx))
            to = walk_of(dy, dx)
            copy = pltpu.make_async_remote_copy(
                src_ref=outgoing.at[pl.ds(pl.multiple_of(to * 128, 128), 128), :],
                dst_ref=incoming.at[at],
                send_sem=red_send.at[at],
                recv_sem=red_recv.at[at],
                device_id={"walk": to},
                device_id_type=MESH,
            )
            copy.start()
            sends.append(copy)
    inv_gather.drain()
    occ_gather.drain()
    total = own
    for copy, (dy, dx) in zip(sends[::-1], [s for s in steps][::-1]):
        at = steps.index((dy, dx))
        copy.wait()
        total = total + incoming[at].astype(jnp.float32)
    out_ref[...] = total


def body(coefficients, inverse, cell_index, fraction, energies, weights, occupied):
    vmem = pl.BlockSpec(memory_space=pltpu.VMEM)
    smem = pl.BlockSpec(memory_space=pltpu.SMEM)
    dma = pltpu.SemaphoreType.DMA
    return pl.pallas_call(
        kernel,
        out_shape=jax.ShapeDtypeStruct((128, WIDE), jnp.float32),
        in_specs=[pl.BlockSpec(memory_space=pl.ANY), vmem, vmem, vmem, smem, smem, vmem],
        out_specs=vmem,
        scratch_shapes=[
            pltpu.VMEM((GRID * PLANE, WIDE), jnp.bfloat16),
            pltpu.VMEM((WIDE, GRID * PLANE), jnp.bfloat16),
            pltpu.VMEM((PLANE, N), jnp.float32),
            pltpu.VMEM((PLANE, N), jnp.float32),
            pltpu.VMEM((GRID, N), jnp.float32),
            pltpu.VMEM((GRID, N), jnp.float32),
            pltpu.VMEM((2, GROUP * PLANE, ETILE), jnp.bfloat16),
            pltpu.VMEM((WIDE, N), jnp.bfloat16),
            pltpu.VMEM((WIDE, N), jnp.bfloat16),
            pltpu.VMEM((N, N), jnp.bfloat16),
            pltpu.VMEM((16 * CAP, N), jnp.bfloat16),
            pltpu.VMEM((WIDE, N), jnp.bfloat16),
            pltpu.VMEM((WIDE, 16 * CAP), jnp.bfloat16),
            pltpu.VMEM((WIDE, N), jnp.bfloat16),
            pltpu.VMEM((N, WIDE), jnp.bfloat16),
            pltpu.VMEM((7, 128, WIDE), jnp.bfloat16),
            dma,
            dma((COPIES,)),
            dma((COPIES,)),
            dma((COPIES,)),
            dma((COPIES,)),
            dma((7,)),
            dma((7,)),
        ],
        compiler_params=pltpu.CompilerParams(
            collective_id=0, has_side_effects=True, vmem_limit_bytes=60 * 1024 * 1024
        ),
        name="orbital_gradient",
    )(
        coefficients,
        inverse.reshape(ROWS, N),
        cell_index.reshape(3, N),
        fraction.reshape(3, N),
        energies,
        weights,
        occupied.reshape(1, N),
    )


def solution(mesh):
    in_specs = (
        P(None, "orb"),
        P("walk", "orb", None),
        P("walk", None, None),
        P("walk", None, None),
        P("walk"),
        P("walk"),
        P(),
    )
    out_specs = P("walk", "orb")
    return jax.shard_map(body, mesh=mesh, in_specs=in_specs, out_specs=out_specs, check_vma=False)
```

```python
import jax
import jax.numpy as jnp
from jax import lax
from jax.experimental import pallas as pl
from jax.experimental.pallas import tpu as pltpu
from jax.sharding import PartitionSpec as P

MESH = pl.DeviceIdType.MESH
GRID = 16
N = 1024
WIDE = 256
CAP = 96
ROWS = 64
PLANE = GRID * GRID
ETILE = 512
GROUP = 4
INV_PIECES = 2
OCC_PIECES = 2
ORDER = (
    ("i", "own", "zp", 0),
    ("i", "own", "zm", 1),
    ("i", "own", "zp", 1),
    ("i", "own", "x", 1),
    ("i", "own", "zm", 0),
    ("c", "tab", "", 0),
    ("i", "own", "x", 0),
    ("c", "L", "", 0),
    ("c", "L", "", 1),
    ("c", "L", "", 2),
    ("c", "L", "", 3),
    ("c", "L", "", 4),
    ("c", "L", "", 5),
    ("c", "L", "", 6),
    ("i", "got", "A", 0),
    ("c", "L", "", 7),
    ("i", "got", "B", 1),
    ("c", "mine", "", 0),
    ("o", "own", "zm", 1),
    ("o", "own", "x", 1),
    ("o", "own", "s", 0),
    ("o", "own", "zp", 0),
    ("c", "V", "", 0),
    ("c", "V", "", 1),
    ("c", "V", "", 2),
    ("i", "got", "X", 1),
    ("c", "V", "", 3),
    ("c", "V", "", 4),
    ("i", "got", "A", 1),
    ("i", "got", "X", 0),
    ("i", "got", "B", 0),
    ("i", "own", "s", 0),
    ("o", "own", "x", 0),
    ("c", "V", "", 5),
    ("i", "got", "C", 0),
    ("o", "got", "A", 0),
    ("i", "mate", "", 0),
    ("c", "V", "", 6),
    ("o", "got", "B", 1),
    ("c", "V", "", 7),
    ("i", "got", "D", 1),
    ("o", "own", "zp", 1),
    ("o", "mate", "", 0),
    ("i", "mate", "", 2),
    ("o", "own", "zm", 0),
    ("i", "got", "C", 1),
    ("i", "got", "E", 1),
    ("i", "mate", "", 3),
    ("o", "got", "X", 1),
    ("i", "mate", "", 4),
    ("o", "got", "X", 0),
    ("i", "got", "E", 0),
    ("o", "got", "C", 0),
    ("o", "got", "C", 1),
    ("o", "mate", "", 3),
    ("i", "got", "D", 0),
    ("i", "mate", "", 1),
    ("i", "got", "F", 1),
    ("o", "mate", "", 4),
    ("o", "got", "A", 1),
    ("i", "mate", "", 6),
    ("c", "R", "", 0),
    ("i", "got", "F", 0),
    ("c", "R", "", 1),
    ("o", "got", "B", 0),
    ("i", "mate", "", 5),
    ("o", "mate", "", 1),
    ("i", "mate", "", 7),
    ("c", "R", "", 2),
    ("c", "R", "", 3),
    ("o", "got", "D", 1),
    ("o", "got", "F", 0),
    ("c", "P", "", 0),
    ("o", "got", "E", 1),
    ("o", "got", "D", 0),
    ("o", "mate", "", 2),
    ("o", "got", "E", 0),
    ("c", "P", "", 1),
    ("o", "got", "F", 1),
    ("c", "P", "", 2),
    ("c", "P", "", 3),
    ("c", "Za", "", 0),
    ("o", "mate", "", 6),
    ("o", "mate", "", 5),
    ("o", "mate", "", 7),
    ("c", "Zb", "", 0),
)


NT = (((1,), (1,)), ((), ()))


def dot_nt(left, right):
    return lax.dot_general(left, right, NT, preferred_element_type=jnp.float32)


def dot_nn(left, right):
    return jnp.dot(left, right, preferred_element_type=jnp.float32)


def axis_table(cell, frac):
    remain = 1.0 - frac
    square = frac * frac
    cubed = square * frac
    sixth = 1.0 / 6.0
    values = (
        remain * remain * remain * sixth,
        (3.0 * cubed - 6.0 * square + 4.0) * sixth,
        (-3.0 * cubed + 3.0 * square + 3.0 * frac + 1.0) * sixth,
        cubed * sixth,
    )
    curves = (remain, 3.0 * frac - 2.0, 1.0 - 3.0 * frac, frac)
    tap = (lax.broadcasted_iota(jnp.int32, (GRID, N), 0) - cell + (GRID + 1)) & (GRID - 1)
    value = jnp.zeros((GRID, N), jnp.float32)
    curve = jnp.zeros((GRID, N), jnp.float32)
    for a in range(4):
        hit = tap == a
        value = jnp.where(hit, values[a], value)
        curve = jnp.where(hit, curves[a], curve)
    return value, curve


def slots_of(occ):
    block = occ >> 8
    member = (lax.broadcasted_iota(jnp.int32, (16, N), 0) == block).astype(jnp.float32)
    tiles = [member[:, t * 128 : (t + 1) * 128] for t in range(N // 128)]
    stacked = jnp.concatenate(tiles, axis=0).astype(jnp.bfloat16)
    row = lax.broadcasted_iota(jnp.int32, (128, 256), 0)
    col = lax.broadcasted_iota(jnp.int32, (128, 256), 1)
    upper = jnp.where((row < col) | (col >= 128), 1.0, 0.0).astype(jnp.bfloat16)
    counted = dot_nn(stacked, upper)
    before = jnp.zeros((16, 128), jnp.float32)
    ranks = []
    for t in range(N // 128):
        piece = counted[t * 16 : (t + 1) * 16, :]
        ranks.append(jnp.sum(tiles[t] * (piece[:, :128] + before), axis=0, keepdims=True))
        before = before + piece[:, 128:]
    return block * CAP + jnp.concatenate(ranks, axis=1).astype(jnp.int32)


def one_hot_rows(first, count, which):
    rows = lax.broadcasted_iota(jnp.int32, (count, N), 0) + first
    return jnp.where(rows == which, 1.0, 0.0).astype(jnp.bfloat16)


class Gather:
    KINDS = "ABXCDEF"
    SPOTS = {"O": (0, 0), "A": (0, 3), "B": (0, 1), "X": (1, 0), "C": (0, 2), "D": (1, 3), "E": (1, 1), "F": (1, 2)}

    def __init__(self, own, buf, rows, pieces, send, recv, place):
        self.own_ref, self.buf, self.rows, self.pieces = own, buf, rows, pieces
        self.send, self.recv = send, recv
        self.xh, self.z, self.c = place
        self.started = []
        self.seen = {}

    @staticmethod
    def copies(pieces):
        return 7 * pieces + 8

    def block(self, kind, piece=None, mate=0):
        dx, dz = self.SPOTS[kind]
        xh = 1 - self.xh if dx else self.xh
        c = 1 - self.c if mate else self.c
        z = (self.z + dz) % 4
        first = (xh * 8 + z * 2 + c) * self.rows
        size = self.rows
        if piece is not None:
            size = self.rows // self.pieces
            first = first + piece * size
        return self.buf.at[pl.ds(pl.multiple_of(first, 8), size), :]

    def device(self, name):
        xh, z, c = self.xh, self.z, self.c
        if name == "zp":
            z = (z + 1) % 4
        if name == "zm":
            z = (z + 3) % 4
        if name == "x":
            xh = 1 - xh
        if name == "s":
            c = 1 - c
        return {"orb": xh * 8 + z * 2 + c}

    def copy(self, src, dst, to, at):
        return pltpu.make_async_remote_copy(
            src_ref=src,
            dst_ref=dst,
            send_sem=self.send.at[at],
            recv_sem=self.recv.at[at],
            device_id=self.device(to),
            device_id_type=MESH,
        )

    def push(self, src, dst, to, at):
        copy = self.copy(src, dst, to, at)
        copy.start()
        self.started.append(copy)

    def index(self, kind, piece):
        return self.KINDS.index(kind) * self.pieces + piece

    def own(self, to, piece):
        if to == "s":
            self.push(self.own_ref, self.block("O"), "s", 7 * self.pieces)
            return
        size = self.rows // self.pieces
        src = self.own_ref.at[pl.ds(piece * size, size), :]
        kind = {"zp": "A", "zm": "B", "x": "X"}[to]
        self.push(src, self.block("O", piece), to, self.index(kind, piece))

    def got(self, kind, piece):
        here = self.block(kind, piece)
        frm = {"A": "zm", "B": "zp", "D": "zm", "E": "zp", "X": "x", "F": "x"}.get(kind)
        if frm is None:
            frm = "zm" if piece < self.pieces // 2 else "zp"
        self.copy(here, here, frm, self.index(kind, piece)).wait_recv()
        if kind == "A" and piece < self.pieces // 2:
            self.push(here, here, "zp", self.index("C", piece))
        if kind == "B" and piece >= self.pieces // 2:
            self.push(here, here, "zm", self.index("C", piece))
        if kind == "X":
            self.push(here, here, "zp", self.index("D", piece))
            self.push(here, here, "zm", self.index("E", piece))
        if kind == "C":
            self.push(here, here, "x", self.index("F", piece))
        self.seen[kind] = self.seen.get(kind, 0) + 1
        if self.seen[kind] == self.pieces:
            whole = self.block(kind)
            self.push(whole, whole, "s", 7 * self.pieces + 1 + self.KINDS.index(kind))

    def mate(self, _, which):
        here = self.block("OABXCDEF"[which], None, 1)
        self.copy(here, here, "s", 7 * self.pieces + which).wait_recv()

    def drain(self):
        for copy in self.started:
            copy.wait_send()


def kernel(
    coef_hbm,
    inv_hbm,
    cell_hbm,
    frac_hbm,
    energy_ref,
    weight_ref,
    occ_hbm,
    out_ref,
    coef,
    inv_ref,
    cell_ref,
    frac_ref,
    occ_ref,
    coef_t,
    plane_val,
    plane_lap,
    x_val,
    x_lap,
    stage,
    total,
    lap_t,
    val_t,
    inv_all,
    occ_all,
    ratio_t,
    slot_t,
    partial,
    y_t,
    outgoing,
    incoming,
    load_sem,
    inv_send,
    inv_recv,
    occ_send,
    occ_recv,
    red_send,
    red_recv,
):
    walk, orb = lax.axis_index("walk"), lax.axis_index("orb")
    yy, xl = walk // 2, walk % 2
    place = (orb // 8, (orb // 2) % 4, orb % 2)
    loads = []
    for at, (src, dst) in enumerate(
        (
            (inv_hbm, inv_ref),
            (cell_hbm, cell_ref),
            (frac_hbm, frac_ref),
            (occ_hbm, occ_ref),
            (coef_hbm, coef),
        )
    ):
        loads.append(pltpu.make_async_copy(src, dst, load_sem.at[at]))
        loads[-1].start()
    mine = occ_all.at[pl.ds(pl.multiple_of(orb * CAP, 16), CAP), :]
    gathers = {
        "i": Gather(inv_ref, inv_all, ROWS, INV_PIECES, inv_send, inv_recv, place),
        "o": Gather(mine, occ_all, CAP, OCC_PIECES, occ_send, occ_recv, place),
    }
    steps = ((2, 1), (2, 0), (1, 1), (1, 0), (3, 1), (3, 0), (0, 1))

    def walk_of(dy, dx):
        return ((yy + dy) % 4) * 2 + (1 - xl if dx else xl)

    barrier = pltpu.get_barrier_semaphore()
    for name in ("zp", "zm", "x", "s"):
        pl.semaphore_signal(
            barrier, inc=1, device_id=gathers["i"].device(name), device_id_type=MESH
        )
    for dy, dx in steps:
        pl.semaphore_signal(
            barrier, inc=1, device_id={"walk": walk_of(dy, dx)}, device_id_type=MESH
        )
    pl.semaphore_wait(barrier, 4 + len(steps))
    for load in loads[:4]:
        load.wait()

    weight = weight_ref[0]
    scaled = weight * energy_ref[0]
    half = 0.5 * weight
    kept = {}

    def tables():
        bx, cx = axis_table(cell_ref[0], frac_ref[0])
        by, cy = axis_table(cell_ref[1], frac_ref[1])
        bz, cz = axis_table(cell_ref[2], frac_ref[2])
        x_val[...] = bx
        x_lap[...] = cx
        for y in range(GRID):
            rows = slice(y * GRID, (y + 1) * GRID)
            plane_val[rows, :] = by[y : y + 1, :] * bz
            plane_lap[rows, :] = cy[y : y + 1, :] * bz + by[y : y + 1, :] * cz
        inv_all[pl.ds(pl.multiple_of(orb * ROWS, 16), ROWS), :] = inv_ref[...]
        loads[4].wait()
        for x in range(GRID):
            points = slice(x * PLANE, (x + 1) * PLANE)
            coef_t[:, points] = coef[points, :].T

    def spline(step, lap):
        t, g = step // (GRID // GROUP), step % (GRID // GROUP)
        cols = slice(t * ETILE, (t + 1) * ETILE)
        at = g % 2
        for k in range(GROUP):
            x = g * GROUP + k
            if lap:
                piece = (
                    x_lap[x : x + 1, cols] * plane_val[:, cols]
                    + x_val[x : x + 1, cols] * plane_lap[:, cols]
                )
            else:
                piece = x_val[x : x + 1, cols] * plane_val[:, cols]
            stage[at, k * PLANE : (k + 1) * PLANE, :] = piece.astype(jnp.bfloat16)
        part = dot_nn(coef_t[:, g * GROUP * PLANE : (g + 1) * GROUP * PLANE], stage[at])
        if g:
            part = part + total[...]
        if g == GRID // GROUP - 1:
            (lap_t if lap else val_t)[:, cols] = part.astype(jnp.bfloat16)
        else:
            total[...] = part

    def pick_occupied():
        occ = occ_ref[...]
        kept["slot"] = slots_of(occ)
        pick = dot_nt(
            one_hot_rows(orb * CAP, CAP, kept["slot"]), one_hot_rows(orb * WIDE, WIDE, occ)
        )
        mine[...] = dot_nn(pick.astype(jnp.bfloat16), lap_t[...]).astype(jnp.bfloat16)

    def side_of(far):
        return 1 - place[0] if far else place[0]

    def ratio_step(t):
        first = pl.multiple_of(side_of(t // 2) * 512 + (t % 2) * 256, 256)
        rows = pl.ds(first, 256)
        ratio_t[:, rows] = dot_nt(val_t[...], inv_all[rows, :]).astype(jnp.bfloat16)

    def slot_step(t):
        first = pl.multiple_of(side_of(t // 2) * 8 * CAP + (t % 2) * 4 * CAP, 4 * CAP)
        hot = one_hot_rows(first, 4 * CAP, kept["slot"])
        slot_t[:, pl.ds(first, 4 * CAP)] = dot_nt(ratio_t[...], hot).astype(jnp.bfloat16)

    def couple(far):
        spots = pl.ds(pl.multiple_of(side_of(far) * 8 * CAP, 8 * CAP), 8 * CAP)
        for cols in tiles:
            part = dot_nn(slot_t[:, spots], occ_all[spots, cols])
            if not far:
                partial[:, cols] = (
                    scaled * val_t[:, cols].astype(jnp.float32)
                    + half * (part - lap_t[:, cols].astype(jnp.float32))
                )
            else:
                y_t[:, cols] = (partial[:, cols] + half * part).astype(jnp.bfloat16)

    tiles = [slice(t * ETILE, (t + 1) * ETILE) for t in range(N // ETILE)]
    work = {
        "tab": lambda k: tables(),
        "L": lambda k: spline(k, True),
        "V": lambda k: spline(k, False),
        "mine": lambda k: pick_occupied(),
        "R": ratio_step,
        "P": slot_step,
        "Za": lambda k: couple(False),
        "Zb": lambda k: couple(True),
    }
    for what, name, kind, k in ORDER:
        if what == "c":
            work[name](k)
        else:
            getattr(gathers[what], name)(kind, k)

    sends = []
    own = None
    for pair in ((2, 1), (3, 0)):
        firsts = [pl.multiple_of(((yy + dy) % 4) * 256, 256) for dy in pair]
        terms = [dot_nt(inv_all[pl.ds(first, 256), :], y_t[...]) for first in firsts]
        for first, term in zip(firsts, terms):
            outgoing[pl.ds(first, 256), :] = term.astype(jnp.bfloat16)
        for dy, term in zip(pair, terms):
            for dx in (1, 0):
                if (dy, dx) == (0, 0):
                    own = jnp.where(xl == 0, term[:128, :], term[128:, :])
                    continue
                at = steps.index((dy, dx))
                to = walk_of(dy, dx)
                copy = pltpu.make_async_remote_copy(
                    src_ref=outgoing.at[pl.ds(pl.multiple_of(to * 128, 128), 128), :],
                    dst_ref=incoming.at[at],
                    send_sem=red_send.at[at],
                    recv_sem=red_recv.at[at],
                    device_id={"walk": to},
                    device_id_type=MESH,
                )
                copy.start()
                sends.append(copy)
    for gather in gathers.values():
        gather.drain()
    result = own
    for copy, (dy, dx) in zip(sends[::-1], [s for s in steps][::-1]):
        at = steps.index((dy, dx))
        copy.wait()
        result = result + incoming[at].astype(jnp.float32)
    out_ref[...] = result


def body(coefficients, inverse, cell_index, fraction, energies, weights, occupied):
    vmem = pl.BlockSpec(memory_space=pltpu.VMEM)
    smem = pl.BlockSpec(memory_space=pltpu.SMEM)
    hbm = pl.BlockSpec(memory_space=pl.ANY)
    dma = pltpu.SemaphoreType.DMA
    return pl.pallas_call(
        kernel,
        out_shape=jax.ShapeDtypeStruct((128, WIDE), jnp.float32),
        in_specs=[hbm, hbm, hbm, hbm, smem, smem, hbm],
        out_specs=vmem,
        scratch_shapes=[
            pltpu.VMEM((GRID * PLANE, WIDE), jnp.bfloat16),
            pltpu.VMEM((ROWS, N), jnp.bfloat16),
            pltpu.VMEM((3, 1, N), jnp.int32),
            pltpu.VMEM((3, 1, N), jnp.float32),
            pltpu.VMEM((1, N), jnp.int32),
            pltpu.VMEM((WIDE, GRID * PLANE), jnp.bfloat16),
            pltpu.VMEM((PLANE, N), jnp.float32),
            pltpu.VMEM((PLANE, N), jnp.float32),
            pltpu.VMEM((GRID, N), jnp.float32),
            pltpu.VMEM((GRID, N), jnp.float32),
            pltpu.VMEM((2, GROUP * PLANE, ETILE), jnp.bfloat16),
            pltpu.VMEM((WIDE, ETILE), jnp.float32),
            pltpu.VMEM((WIDE, N), jnp.bfloat16),
            pltpu.VMEM((WIDE, N), jnp.bfloat16),
            pltpu.VMEM((N, N), jnp.bfloat16),
            pltpu.VMEM((16 * CAP, N), jnp.bfloat16),
            pltpu.VMEM((WIDE, N), jnp.bfloat16),
            pltpu.VMEM((WIDE, 16 * CAP), jnp.bfloat16),
            pltpu.VMEM((WIDE, N), jnp.float32),
            pltpu.VMEM((WIDE, N), jnp.bfloat16),
            pltpu.VMEM((N, WIDE), jnp.bfloat16),
            pltpu.VMEM((7, 128, WIDE), jnp.bfloat16),
            dma((5,)),
            dma((Gather.copies(INV_PIECES),)),
            dma((Gather.copies(INV_PIECES),)),
            dma((Gather.copies(OCC_PIECES),)),
            dma((Gather.copies(OCC_PIECES),)),
            dma((7,)),
            dma((7,)),
        ],
        compiler_params=pltpu.CompilerParams(
            collective_id=0, has_side_effects=True, vmem_limit_bytes=60 * 1024 * 1024
        ),
        name="orbital_gradient",
    )(
        coefficients,
        inverse.reshape(ROWS, N),
        jnp.transpose(cell_index, (1, 0, 2)),
        jnp.transpose(fraction, (1, 0, 2)),
        energies,
        weights,
        occupied.reshape(1, N),
    )


def solution(mesh):
    in_specs = (
        P(None, "orb"),
        P("walk", "orb", None),
        P("walk", None, None),
        P("walk", None, None),
        P("walk"),
        P("walk"),
        P(),
    )
    out_specs = P("walk", "orb")
    return jax.shard_map(body, mesh=mesh, in_specs=in_specs, out_specs=out_specs, check_vma=False)
```
